256 devices in a mesh: gx: 16 (over z, core), gy: 16 (over x, y).
Axes of the slice: x: 4, y: 4, z: 8, core: 2. Of those that a mesh axis runs over, the one named last changes fastest.
Arguments:
- tokens: bfloat16 [4096, 4096], P('gx', 'gy'), may hold values from -6 to 6
- gate_blocks: bfloat16 [16, 16, 10, 128, 128], P('gy', 'gx'), may hold values from -0.125 to 0.125
- up_blocks: bfloat16 [16, 16, 10, 128, 128], P('gy', 'gx'), may hold values from -0.125 to 0.125
- gate_coords: int32 [16, 16, 10, 2], P('gy', 'gx'), may hold values from 0 to 6, as said below
- gate_count: int32 [16, 16], P('gy', 'gx'), may hold values from 3 to 10, as said below
- down_blocks: bfloat16 [16, 16, 6, 128, 128], P('gx', 'gy'), may hold values from -0.09375 to 0.09375
- down_rows: int32 [16, 16, 4], P('gx'), may hold values from 0 to 6, as said below
- down_coords: int32 [16, 16, 6, 2], P('gx', 'gy'), may hold values from 0 to 3, as said below
- down_count: int32 [16, 16], P('gx', 'gy'), may hold values from 2 to 6, as said below
Outputs:
- mixed: bfloat16 [4096, 4096], P('gx', 'gy')
The draws below stay inside these ranges and needn't reach their ends.
Inputs may be any that keep to these rules, and one draw needn't show every extreme that they name: `gate_coords`: within each tile the 10 (model-width block, hidden block) pairs are distinct, the first below 2, the second below 7; only the first gate_count slots are live. `gate_count`: some tile has all 10 slots live. `down_rows`: within each down tile the 4 hidden blocks are distinct. `down_coords`: within each down tile the 6 (kept-row index below 4, model-width block below 2) pairs are distinct; only the first down_count slots are live. `down_count`: some tile has all 6 slots live.
All inputs are finite; a program needn't handle non-finite values.
Results may differ from the reference program's by a relative error of at most 0.025.
Values may be sent and summed in bfloat16 or wider, within the bound.
No kernel may reach another device: no remote copies, remote signals or barrier semaphores. Data moves between devices by JAX's collectives and lax.ppermute only.
A program may use at most 64 MiB of HBM per device.

```python
import jax
import jax.numpy as jnp
from jax import lax

D = 4096
FF = 14336
BLOCK = 128
TOKENS = 4096
DB = 2
FB = 7
CAP = 10
LOW = 3
USED = 4
CAPD = 6
LOWD = 2
N_GX = 16
N_GY = 16


def tile_pairs(key, tiles, positions, slots, inner):
    tile_keys = jax.random.split(key, tiles)
    orders = jax.vmap(lambda one_key: jax.random.permutation(one_key, positions))(tile_keys)[:, :slots]
    return jnp.stack([orders // inner, orders % inner], -1).astype(jnp.int32)


def tile_counts(key, tiles, lowest, highest):
    counts = jax.random.randint(key, (tiles,), lowest, highest + 1)
    chosen = jax.random.randint(jax.random.fold_in(key, 7), (), 0, tiles)
    return jnp.where(jnp.arange(tiles) == chosen, highest, counts).astype(jnp.int32)


def draw_gate_coords(key, part):
    pairs = tile_pairs(jax.random.fold_in(key, 11), N_GY * N_GX, DB * FB, CAP, FB)
    return pairs.reshape(N_GY, N_GX, CAP, 2)


def draw_gate_count(key, part):
    return tile_counts(jax.random.fold_in(key, 12), N_GY * N_GX, LOW, CAP).reshape(N_GY, N_GX)


def draw_down_rows(key, part):
    tile_keys = jax.random.split(jax.random.fold_in(key, 13), N_GX * N_GY)
    orders = jax.vmap(lambda one_key: jax.random.permutation(one_key, FB))(tile_keys)[:, :USED]
    return orders.astype(jnp.int32).reshape(N_GX, N_GY, USED)


def draw_down_coords(key, part):
    pairs = tile_pairs(jax.random.fold_in(key, 14), N_GX * N_GY, USED * DB, CAPD, DB)
    return pairs.reshape(N_GX, N_GY, CAPD, 2)


def draw_down_count(key, part):
    return tile_counts(jax.random.fold_in(key, 15), N_GX * N_GY, LOWD, CAPD).reshape(N_GX, N_GY)


def shard_levels(rng, shape, cuts, least, high):
    gain, own = 1.0, jax.random.fold_in(rng, 6)
    for dim, shards_of in cuts:
        steps = jnp.exp(jax.random.uniform(jax.random.fold_in(own, dim), (shards_of,), jnp.float32, least / len(cuts), high / len(cuts)))
        gain = gain * jnp.repeat(steps, shape[dim] // shards_of).reshape([-1 if axis == dim else 1 for axis in range(len(shape))])
    return gain


def centred(own_key, extent, scale, limit, cuts=(), held_as=jnp.bfloat16):
    gain = shard_levels(own_key, extent, cuts, -0.22, 0.18) if cuts else 1.0
    values = jax.random.normal(own_key, extent, jnp.float32) * scale * gain
    return jnp.minimum(jnp.maximum(values, -limit), limit).astype(held_as)


def setup_inputs(seed: int = 0) -> dict:
    arg_keys = jax.random.split(jax.random.key(seed), 10)
    tokens = centred(arg_keys[0], (TOKENS, D), 1.0, 6.0, ((0, 16), (1, 16)))
    gate_blocks = centred(arg_keys[1], (N_GY, N_GX, CAP, BLOCK, BLOCK), (D // 2) ** -0.5, 0.125, ((0, 16), (1, 16)))
    up_blocks = centred(arg_keys[2], (N_GY, N_GX, CAP, BLOCK, BLOCK), (D // 2) ** -0.5, 0.125, ((0, 16), (1, 16)))
    gate_coords = draw_gate_coords(jax.random.fold_in(arg_keys[9], 71), 0)
    gate_count = draw_gate_count(jax.random.fold_in(arg_keys[9], 71), 0)
    down_blocks = centred(arg_keys[5], (N_GX, N_GY, CAPD, BLOCK, BLOCK), (FF * 2 // 7) ** -0.5, 0.09375, ((0, 16), (1, 16)))
    down_rows = draw_down_rows(jax.random.fold_in(arg_keys[9], 71), 0)
    down_coords = draw_down_coords(jax.random.fold_in(arg_keys[9], 71), 0)
    down_count = draw_down_count(jax.random.fold_in(arg_keys[9], 71), 0)
    return dict(tokens=tokens, gate_blocks=gate_blocks, up_blocks=up_blocks, gate_coords=gate_coords, gate_count=gate_count, down_blocks=down_blocks, down_rows=down_rows, down_coords=down_coords, down_count=down_count)


def dense_matrix(blocks, local_rows, local_cols, counts, per_row, per_col, row_blocks, col_blocks):
    tiles_a, tiles_b, slots = blocks.shape[0], blocks.shape[1], blocks.shape[2]
    live_slots = jnp.arange(slots, dtype=jnp.int32)[None, None, :] < counts[:, :, None]
    global_rows = jnp.arange(tiles_a, dtype=jnp.int32)[:, None, None] * per_row + local_rows
    global_cols = jnp.arange(tiles_b, dtype=jnp.int32)[None, :, None] * per_col + local_cols
    values = jnp.where(live_slots[..., None, None], blocks, jnp.zeros((), blocks.dtype))
    grid = jnp.zeros((row_blocks, col_blocks, BLOCK, BLOCK), blocks.dtype)
    grid = grid.at[global_rows, global_cols].add(values)
    return grid.transpose(0, 2, 1, 3).reshape(row_blocks * BLOCK, col_blocks * BLOCK)


def rounded_sum(total, term):
    held = lax.optimization_barrier(term.astype(jnp.bfloat16))
    return total + held.astype(jnp.float32)


def reference(tokens, gate_blocks, up_blocks, gate_coords, gate_count, down_blocks, down_rows, down_coords, down_count):
    model_blocks = D // BLOCK
    hidden_blocks = FF // BLOCK
    gate_weight = dense_matrix(gate_blocks, gate_coords[..., 0], gate_coords[..., 1], gate_count, DB, FB, model_blocks, hidden_blocks)
    up_weight = dense_matrix(up_blocks, gate_coords[..., 0], gate_coords[..., 1], gate_count, DB, FB, model_blocks, hidden_blocks)
    kept_rows = jnp.take_along_axis(down_rows, down_coords[..., 0], axis=2)
    down_weight = dense_matrix(down_blocks, kept_rows, down_coords[..., 1], down_count, FB, DB, hidden_blocks, model_blocks)
    gate_total = jnp.zeros((TOKENS, FF), jnp.float32)
    up_total = jnp.zeros((TOKENS, FF), jnp.float32)
    width = DB * BLOCK
    for tile_row in range(N_GY):
        columns = tokens[:, tile_row * width:(tile_row + 1) * width]
        gate_total = rounded_sum(gate_total, jnp.dot(columns, gate_weight[tile_row * width:(tile_row + 1) * width], preferred_element_type=jnp.float32))
        up_total = rounded_sum(up_total, jnp.dot(columns, up_weight[tile_row * width:(tile_row + 1) * width], preferred_element_type=jnp.float32))
    hidden = (jax.nn.silu(gate_total) * up_total).astype(jnp.bfloat16)
    out_total = jnp.zeros((TOKENS, D), jnp.float32)
    span = FB * BLOCK
    for tile_col in range(N_GX):
        part_hidden = hidden[:, tile_col * span:(tile_col + 1) * span]
        out_total = rounded_sum(out_total, jnp.dot(part_hidden, down_weight[tile_col * span:(tile_col + 1) * span], preferred_element_type=jnp.float32))
    return out_total.astype(jnp.bfloat16)
```

```python
import functools

import jax
import jax.numpy as jnp
from jax import lax
from jax.experimental import pallas as pl
from jax.experimental.pallas import tpu as pltpu
from jax.sharding import PartitionSpec as P


BLOCK = 128
SLOTS = 10
DOWN_SLOTS = 6
FB = 7
NZ = 8
RING = 4
GATE_ROWS = SLOTS * BLOCK
DOWN_AT = 2 * GATE_ROWS
META_AT = DOWN_AT + DOWN_SLOTS * BLOCK
MSG_ROWS = META_AT + 16
CHUNK = 32
WIDTH = 256
HID = 2 * FB


VMEM = pl.BlockSpec(memory_space=pltpu.VMEM)
HBM = pl.BlockSpec(memory_space=pltpu.HBM)
SMEM = pl.BlockSpec(memory_space=pltpu.SMEM)
bf16 = jnp.bfloat16


def z_perm(d):
    return [(2 * z + c, 2 * ((z + d) % NZ) + c) for z in range(NZ) for c in range(2)]


def x_perm(d):
    return [(4 * x + y, 4 * ((x + d) % 4) + y) for x in range(4) for y in range(4)]


def y_perm(d):
    return [(4 * x + y, 4 * x + (y + d) % 4) for x in range(4) for y in range(4)]


PARTNER = [(i, i ^ 1) for i in range(16)]


def plane_xy():
    me = lax.axis_index("gy")
    return lax.shift_right_logical(me, 2), me & 3


def call(kernel, specs, out_shape, scratch=(), limit=16, flops=0):
    return pl.pallas_call(
        kernel,
        out_shape=out_shape,
        in_specs=specs,
        out_specs=jax.tree.map(lambda _: VMEM, out_shape),
        scratch_shapes=list(scratch),
        compiler_params=pltpu.CompilerParams(vmem_limit_bytes=limit << 20),
        cost_estimate=pl.CostEstimate(flops=flops, bytes_accessed=0, transcendentals=0),
    )


def shape(*dims, dtype=bf16):
    return jax.ShapeDtypeStruct(dims, dtype)


def split_tokens(tok, *outs):
    x, y = plane_xy()
    for k in range(RING):
        outs[k][...] = tok[(x + k) & 3]
        outs[RING + k][...] = tok[4 + ((y + k) & 3)]


def stack_tokens(*refs):
    out = refs[-1]
    for i in range(2 * RING):
        out[i] = refs[i][...]


def pack_weights(coords, count, rows, down_coords, down_count, gate, up, down, msg, sems):
    me = lax.axis_index("gy")
    copies = [
        pltpu.make_async_copy(gate, msg.at[pl.ds(0, GATE_ROWS)], sems.at[0]),
        pltpu.make_async_copy(up, msg.at[pl.ds(GATE_ROWS, GATE_ROWS)], sems.at[1]),
        pltpu.make_async_copy(down, msg.at[pl.ds(DOWN_AT, DOWN_SLOTS * BLOCK)], sems.at[2]),
    ]
    for c in copies:
        c.start()
    live = count[0, 0]
    down_live = down_count[0, 0]
    lane = lax.broadcasted_iota(jnp.int32, (16, BLOCK), 1)
    meta = jnp.zeros((16, BLOCK), jnp.int32)
    for s in range(SLOTS):
        meta = jnp.where(lane == s, coords[0, s] * FB + coords[1, s], meta)
    for s in range(DOWN_SLOTS):
        row = rows[down_coords[0, s], me]
        meta = jnp.where(lane == SLOTS + s, row * 2 + down_coords[1, s], meta)
    msg[META_AT:MSG_ROWS] = meta.astype(jnp.float32).astype(bf16)
    for c in copies:
        c.wait()
    zero = jnp.zeros((BLOCK, BLOCK), bf16)
    for s in range(SLOTS):

        @pl.when(s >= live)
        def _():
            msg[s * BLOCK : (s + 1) * BLOCK] = zero
            msg[GATE_ROWS + s * BLOCK : GATE_ROWS + (s + 1) * BLOCK] = zero

    for s in range(DOWN_SLOTS):

        @pl.when(s >= down_live)
        def _():
            msg[DOWN_AT + s * BLOCK : DOWN_AT + (s + 1) * BLOCK] = zero


def places(msg):
    return msg[META_AT:MSG_ROWS].astype(jnp.float32).astype(jnp.int32)


def gate_up(half, *refs):
    toks, msgs, outs = refs[:NZ], refs[NZ : 2 * NZ], refs[2 * NZ : 2 * NZ + RING]
    dense, lhs = refs[2 * NZ + RING :]
    x, y = plane_xy()
    v = y if half == 0 else x
    for j in range(NZ):
        k = (j // 2 - v) & 3
        for d in range(RING):
            lhs[2 * k + j % 2, :, d * WIDTH : (d + 1) * WIDTH] = toks[j][half * RING + d]

    @pl.loop(0, HID)
    def _(n):
        dense[n] = jnp.zeros(dense.shape[1:], bf16)

    for i in range(2 * RING):
        d, core = i // 2, i % 2
        meta = places(msgs[i])
        for s in range(SLOTS):
            p = meta[0, s]
            r = (p >= FB).astype(jnp.int32)
            at = core * FB + p - FB * r
            dense[at, 2 * d + r, :, :BLOCK] = msgs[i][s * BLOCK : (s + 1) * BLOCK]
            dense[at, 2 * d + r, :, BLOCK:] = msgs[i][
                GATE_ROWS + s * BLOCK : GATE_ROWS + (s + 1) * BLOCK
            ]

    left = lhs[...].reshape(NZ * CHUNK, RING * WIDTH)

    @pl.loop(0, HID)
    def _(n):
        part = jnp.dot(
            left, dense[n].reshape(RING * WIDTH, WIDTH), preferred_element_type=jnp.float32
        ).astype(bf16)
        for k in range(RING):
            outs[k][n] = part[2 * CHUNK * k : 2 * CHUNK * (k + 1)]


def activate(*refs):
    out = refs[RING]
    total = refs[0][...].astype(jnp.float32)
    for k in range(1, RING):
        total = total + refs[k][...].astype(jnp.float32)
    gate, up = total[:, :, :BLOCK], total[:, :, BLOCK:]
    out[...] = (gate / (1.0 + jnp.exp(-gate)) * up).astype(bf16)


def spread_down(*refs):
    msgs, out = refs[: 2 * RING], refs[-1]
    for d in range(RING):
        out[d] = jnp.zeros(out.shape[1:], bf16)
    for i in range(2 * RING):
        d, core = i // 2, i % 2
        meta = places(msgs[i])
        for s in range(DOWN_SLOTS):
            q = meta[0, SLOTS + s]
            row = lax.shift_right_logical(q, 1)
            col = pl.multiple_of((q & 1) * BLOCK, BLOCK)
            out[d, core * FB + row, :, pl.ds(col, BLOCK)] = msgs[i][
                DOWN_AT + s * BLOCK : DOWN_AT + (s + 1) * BLOCK
            ]


def down(*refs):
    hids, dense, outs, lefts = refs[: 2 * RING], refs[2 * RING : 2 * RING + 2], refs[10:18], refs[18:]
    x, y = plane_xy()
    for half in range(2):
        v = y if half == 0 else x
        lhs = lefts[half]
        for d in range(RING):
            at = (v - d) & 3
            for n in range(HID):
                lhs[at, :, n * BLOCK : (n + 1) * BLOCK] = hids[half * RING + d][n]
    for half in range(2):
        left = lefts[half][...].reshape(NZ * CHUNK, HID * BLOCK)

        @pl.loop(0, RING)
        def _(d):
            part = jnp.dot(
                left,
                dense[half][d].reshape(HID * BLOCK, WIDTH),
                preferred_element_type=jnp.float32,
            ).astype(bf16)
            for j in range(NZ):
                outs[j][half * RING + d] = part[CHUNK * j : CHUNK * (j + 1)]


def add_up(*refs):
    ins, outs = refs[:NZ], refs[NZ:]
    for i in range(2 * RING):
        total = ins[0][i].astype(jnp.float32)
        for j in range(1, NZ):
            total = total + ins[j][i].astype(jnp.float32)
        outs[i][...] = total.astype(bf16)


def place(*refs):
    out = refs[-1]
    x, y = plane_xy()
    for d in range(RING):
        out[(x + d) & 3] = refs[d][...]
        out[4 + ((y + d) & 3)] = refs[RING + d][...]


def body(
    tokens,
    gate_blocks,
    up_blocks,
    gate_coords,
    gate_count,
    down_blocks,
    down_rows,
    down_coords,
    down_count,
):
    perms = (x_perm, y_perm)

    small = call(split_tokens, [VMEM], [shape(CHUNK, WIDTH)] * 8)(tokens.reshape(8, CHUNK, WIDTH))
    pieces = []
    for half in range(2):
        pieces.append(small[half * RING])
        for d in range(1, RING):
            pieces.append(lax.ppermute(small[half * RING + d], "gy", perms[half](d)))
    mine = call(stack_tokens, [VMEM] * 8, shape(8, CHUNK, WIDTH))(*pieces)
    toks = [mine] + [lax.ppermute(mine, "gx", z_perm(j)) for j in range(1, NZ)]

    msg = call(
        pack_weights,
        [SMEM] * 5 + [HBM] * 3,
        shape(MSG_ROWS, BLOCK),
        scratch=[pltpu.SemaphoreType.DMA((3,))],
    )(
        gate_coords[0, 0].T,
        gate_count,
        down_rows[0].T,
        down_coords[0, 0].T,
        down_count,
        gate_blocks.reshape(GATE_ROWS, BLOCK),
        up_blocks.reshape(GATE_ROWS, BLOCK),
        down_blocks.reshape(DOWN_SLOTS * BLOCK, BLOCK),
    )
    own_pair = (msg, lax.ppermute(msg, "gx", PARTNER))
    weights = []
    for half in range(2):
        group = list(own_pair)
        for d in range(1, RING):
            got = lax.ppermute(msg, "gy", perms[half](d))
            group += [got, lax.ppermute(got, "gx", PARTNER)]
        weights.append(group)

    hidden = []
    dense_down = []
    for half in range(2):
        part = call(
            functools.partial(gate_up, half),
            [VMEM] * (2 * NZ),
            [shape(HID, 2 * CHUNK, WIDTH)] * RING,
            scratch=[
                pltpu.VMEM((HID, 2 * RING, BLOCK, WIDTH), bf16),
                pltpu.VMEM((NZ, CHUNK, RING * WIDTH), bf16),
            ],
            limit=20,
            flops=2 * 256 * 1024 * 3584,
        )(*toks, *weights[half])
        got = [part[0]] + [lax.ppermute(part[d], "gy", perms[1 - half](d)) for d in range(1, RING)]
        dense_down.append(
            call(
                spread_down,
                [VMEM] * (2 * RING),
                shape(RING, HID, BLOCK, WIDTH),
                limit=12,
                flops=10**9,
            )(*weights[half])
        )
        h = call(activate, [VMEM] * RING, shape(HID, 2 * CHUNK, BLOCK))(*got)
        hidden += [h] + [lax.ppermute(h, "gy", perms[1 - half](d)) for d in range(1, RING)]
    partial = call(
        down,
        [VMEM] * (2 * RING + 2),
        [shape(8, CHUNK, WIDTH)] * NZ,
        scratch=[pltpu.VMEM((RING, 2 * CHUNK, HID * BLOCK), bf16)] * 2,
        flops=2 * 2 * 256 * 1792 * 1024,
    )(*hidden, *dense_down)
    got = [partial[0]] + [lax.ppermute(partial[j], "gx", z_perm(-j)) for j in range(1, NZ)]
    sums = call(add_up, [VMEM] * NZ, [shape(CHUNK, WIDTH)] * 8)(*got)
    final = []
    for half in range(2):
        final.append(sums[half * RING])
        for d in range(1, RING):
            final.append(lax.ppermute(sums[half * RING + d], "gy", perms[half](-d)))
    out = call(place, [VMEM] * 8, shape(8, CHUNK, WIDTH))(*final)
    return out.reshape(tokens.shape)


def solution(mesh):
    return jax.shard_map(
        body,
        mesh=mesh,
        in_specs=(
            P("gx", "gy"),
            P("gy", "gx", None, None, None),
            P("gy", "gx", None, None, None),
            P("gy", "gx", None, None),
            P("gy", "gx"),
            P("gx", "gy", None, None, None),
            P("gx", None, None),
            P("gx", "gy", None, None),
            P("gx", "gy"),
        ),
        out_specs=P("gx", "gy"),
        check_vma=False,
    )
```

```python
import functools

import jax
import jax.numpy as jnp
from jax import lax
from jax.experimental import pallas as pl
from jax.experimental.pallas import tpu as pltpu
from jax.sharding import PartitionSpec as P


BLOCK = 128
SLOTS = 10
DOWN_SLOTS = 6
FB = 7
NZ = 8
RING = 4
GATE_ROWS = SLOTS * BLOCK
DOWN_AT = 2 * GATE_ROWS
META_AT = DOWN_AT + DOWN_SLOTS * BLOCK
MSG_ROWS = META_AT + 16
CHUNK = 32
WIDTH = 256
HID = 2 * FB


VMEM = pl.BlockSpec(memory_space=pltpu.VMEM)
HBM = pl.BlockSpec(memory_space=pltpu.HBM)
SMEM = pl.BlockSpec(memory_space=pltpu.SMEM)
bf16 = jnp.bfloat16


def z_perm(d):
    return [(2 * z + c, 2 * ((z + d) % NZ) + c) for z in range(NZ) for c in range(2)]


def x_perm(d):
    return [(4 * x + y, 4 * ((x + d) % 4) + y) for x in range(4) for y in range(4)]


def y_perm(d):
    return [(4 * x + y, 4 * x + (y + d) % 4) for x in range(4) for y in range(4)]


PARTNER = [(i, i ^ 1) for i in range(16)]


def plane_xy():
    me = lax.axis_index("gy")
    return lax.shift_right_logical(me, 2), me & 3


def call(kernel, specs, out_shape, scratch=(), limit=16, flops=0):
    return pl.pallas_call(
        kernel,
        out_shape=out_shape,
        in_specs=specs,
        out_specs=jax.tree.map(lambda _: VMEM, out_shape),
        scratch_shapes=list(scratch),
        compiler_params=pltpu.CompilerParams(vmem_limit_bytes=limit << 20),
        cost_estimate=pl.CostEstimate(flops=flops, bytes_accessed=0, transcendentals=0),
    )


def shape(*dims, dtype=bf16):
    return jax.ShapeDtypeStruct(dims, dtype)


def split_tokens(tok, out):
    x, y = plane_xy()
    out[...] = jnp.zeros_like(out)
    for k in range(1, RING):
        u, w = (x + k) & 3, (y + k) & 3
        out[4 * u + y] = tok[u]
        out[4 * x + w] = tok[4 + w]


def stack_tokens(tok, got, out):
    x, y = plane_xy()
    out[0] = tok[x]
    out[RING] = tok[4 + y]
    for d in range(1, RING):
        out[d] = got[4 * ((x - d) & 3) + y]
        out[RING + d] = got[4 * x + ((y - d) & 3)]


def pack_weights(coords, count, rows, down_coords, down_count, gate, up, down, msg, sems):
    me = lax.axis_index("gy")
    copies = [
        pltpu.make_async_copy(gate, msg.at[pl.ds(0, GATE_ROWS)], sems.at[0]),
        pltpu.make_async_copy(up, msg.at[pl.ds(GATE_ROWS, GATE_ROWS)], sems.at[1]),
        pltpu.make_async_copy(down, msg.at[pl.ds(DOWN_AT, DOWN_SLOTS * BLOCK)], sems.at[2]),
    ]
    for c in copies:
        c.start()
    live = count[0, 0]
    down_live = down_count[0, 0]
    lane = lax.broadcasted_iota(jnp.int32, (16, BLOCK), 1)
    meta = jnp.zeros((16, BLOCK), jnp.int32)
    for s in range(SLOTS):
        meta = jnp.where(lane == s, coords[0, s] * FB + coords[1, s], meta)
    for s in range(DOWN_SLOTS):
        row = rows[down_coords[0, s], me]
        meta = jnp.where(lane == SLOTS + s, row * 2 + down_coords[1, s], meta)
    msg[META_AT:MSG_ROWS] = meta.astype(jnp.float32).astype(bf16)
    for c in copies:
        c.wait()
    zero = jnp.zeros((BLOCK, BLOCK), bf16)
    for s in range(SLOTS):

        @pl.when(s >= live)
        def _():
            msg[s * BLOCK : (s + 1) * BLOCK] = zero
            msg[GATE_ROWS + s * BLOCK : GATE_ROWS + (s + 1) * BLOCK] = zero

    for s in range(DOWN_SLOTS):

        @pl.when(s >= down_live)
        def _():
            msg[DOWN_AT + s * BLOCK : DOWN_AT + (s + 1) * BLOCK] = zero


def places(msg):
    return msg[META_AT:MSG_ROWS].astype(jnp.float32).astype(jnp.int32)


def gate_up(half, *refs):
    toks, msgs, outs = refs[:NZ], refs[NZ : 2 * NZ], refs[2 * NZ : 2 * NZ + RING]
    dense, lhs, at = refs[2 * NZ + RING :]
    x, y = plane_xy()
    v = y if half == 0 else x
    for j in range(NZ):
        k = (j // 2 - v) & 3
        for d in range(RING):
            lhs[2 * k + j % 2, :, d * WIDTH : (d + 1) * WIDTH] = toks[j][half * RING + d]

    @pl.loop(0, HID)
    def _(n):
        dense[n] = jnp.zeros(dense.shape[1:], bf16)

    for i in range(2 * RING):
        meta = places(msgs[i])
        for s in range(SLOTS):
            at[i, s] = meta[0, s]
    for i in range(2 * RING):
        d, core = i // 2, i % 2

        def put(s, carry):
            p = at[i, s]
            r = (p >= FB).astype(jnp.int32)
            col = core * FB + p - FB * r
            src = pl.multiple_of(s * BLOCK, BLOCK)
            dense[col, 2 * d + r, :, :BLOCK] = msgs[i][pl.ds(src, BLOCK), :]
            dense[col, 2 * d + r, :, BLOCK:] = msgs[i][pl.ds(GATE_ROWS + src, BLOCK), :]
            return carry

        lax.fori_loop(0, SLOTS, put, 0, unroll=2)

    left = lhs[...].reshape(NZ * CHUNK, RING * WIDTH)

    @pl.loop(0, HID)
    def _(n):
        part = jnp.dot(
            left, dense[n].reshape(RING * WIDTH, WIDTH), preferred_element_type=jnp.float32
        ).astype(bf16)
        for k in range(RING):
            outs[k][n] = part[2 * CHUNK * k : 2 * CHUNK * (k + 1)]


def activate(*refs):
    out = refs[RING]

    @pl.loop(0, HID)
    def _(n):
        total = refs[0][n].astype(jnp.float32)
        for k in range(1, RING):
            total = total + refs[k][n].astype(jnp.float32)
        gate, up = total[:, :BLOCK], total[:, BLOCK:]
        out[n] = (gate / (1.0 + jnp.exp(-gate)) * up).astype(bf16)


def spread_down(*refs):
    msgs, out = refs[: 2 * RING], refs[-1]
    for d in range(RING):
        out[d] = jnp.zeros(out.shape[1:], bf16)
    for i in range(2 * RING):
        d, core = i // 2, i % 2
        meta = places(msgs[i])
        for s in range(DOWN_SLOTS):
            q = meta[0, SLOTS + s]
            row = lax.shift_right_logical(q, 1)
            col = pl.multiple_of((q & 1) * BLOCK, BLOCK)
            out[d, core * FB + row, :, pl.ds(col, BLOCK)] = msgs[i][
                DOWN_AT + s * BLOCK : DOWN_AT + (s + 1) * BLOCK
            ]


def down(*refs):
    hids, dense, outs, lefts = refs[: 2 * RING], refs[2 * RING : 2 * RING + 2], refs[10:18], refs[18:]
    x, y = plane_xy()
    for half in range(2):
        v = y if half == 0 else x
        lhs = lefts[half]
        for d in range(RING):
            at = (v - d) & 3
            for n in range(HID):
                lhs[at, :, n * BLOCK : (n + 1) * BLOCK] = hids[half * RING + d][n]
    for half in range(2):
        left = lefts[half][...].reshape(NZ * CHUNK, HID * BLOCK)

        @pl.loop(0, RING)
        def _(d):
            part = jnp.dot(
                left,
                dense[half][d].reshape(HID * BLOCK, WIDTH),
                preferred_element_type=jnp.float32,
            ).astype(bf16)
            for j in range(NZ):
                outs[j][half * RING + d] = part[CHUNK * j : CHUNK * (j + 1)]


def add_up(*refs):
    ins, outs = refs[:NZ], refs[NZ:]
    for i in range(2 * RING):
        total = ins[0][i].astype(jnp.float32)
        for j in range(1, NZ):
            total = total + ins[j][i].astype(jnp.float32)
        outs[i][...] = total.astype(bf16)


def place(*refs):
    out = refs[-1]
    x, y = plane_xy()
    for d in range(RING):
        out[(x + d) & 3] = refs[d][...]
        out[4 + ((y + d) & 3)] = refs[RING + d][...]


def body(
    tokens,
    gate_blocks,
    up_blocks,
    gate_coords,
    gate_count,
    down_blocks,
    down_rows,
    down_coords,
    down_count,
):
    perms = (x_perm, y_perm)

    tok = tokens.reshape(8, CHUNK, WIDTH)
    small = lax.all_to_all(
        call(split_tokens, [VMEM], shape(16, CHUNK, WIDTH))(tok),
        "gy", 0, 0, tiled=True,
    )
    mine = call(stack_tokens, [VMEM] * 2, shape(8, CHUNK, WIDTH))(tok, small)
    toks = [mine] + [lax.ppermute(mine, "gx", z_perm(j)) for j in range(1, NZ)]

    msg = call(
        pack_weights,
        [SMEM] * 5 + [HBM] * 3,
        shape(MSG_ROWS, BLOCK),
        scratch=[pltpu.SemaphoreType.DMA((3,))],
    )(
        gate_coords[0, 0].T,
        gate_count,
        down_rows[0].T,
        down_coords[0, 0].T,
        down_count,
        gate_blocks.reshape(GATE_ROWS, BLOCK),
        up_blocks.reshape(GATE_ROWS, BLOCK),
        down_blocks.reshape(DOWN_SLOTS * BLOCK, BLOCK),
    )
    own_pair = (msg, lax.ppermute(msg, "gx", PARTNER))
    weights = []
    for half in range(2):
        group = list(own_pair)
        for d in range(1, RING):
            got = lax.ppermute(msg, "gy", perms[half](d))
            group += [got, lax.ppermute(got, "gx", PARTNER)]
        weights.append(group)

    hidden = []
    dense_down = []
    for half in range(2):
        part = call(
            functools.partial(gate_up, half),
            [VMEM] * (2 * NZ),
            [shape(HID, 2 * CHUNK, WIDTH)] * RING,
            scratch=[
                pltpu.VMEM((HID, 2 * RING, BLOCK, WIDTH), bf16),
                pltpu.VMEM((NZ, CHUNK, RING * WIDTH), bf16),
                pltpu.SMEM((2 * RING, SLOTS), jnp.int32),
            ],
            limit=20,
            flops=2 * 256 * 1024 * 3584,
        )(*toks, *weights[half])
        got = [part[0]] + [lax.ppermute(part[d], "gy", perms[1 - half](d)) for d in range(1, RING)]
        dense_down.append(
            call(
                spread_down,
                [VMEM] * (2 * RING),
                shape(RING, HID, BLOCK, WIDTH),
                limit=12,
                flops=10**9,
            )(*weights[half])
        )
        h = call(activate, [VMEM] * RING, shape(HID, 2 * CHUNK, BLOCK))(*got)
        hidden += [h] + [lax.ppermute(h, "gy", perms[1 - half](d)) for d in range(1, RING)]
    partial = call(
        down,
        [VMEM] * (2 * RING + 2),
        [shape(8, CHUNK, WIDTH)] * NZ,
        scratch=[pltpu.VMEM((RING, 2 * CHUNK, HID * BLOCK), bf16)] * 2,
        flops=2 * 2 * 256 * 1792 * 1024,
    )(*hidden, *dense_down)
    got = [partial[0]] + [lax.ppermute(partial[j], "gx", z_perm(-j)) for j in range(1, NZ)]
    sums = call(add_up, [VMEM] * NZ, [shape(CHUNK, WIDTH)] * 8)(*got)
    final = []
    for half in range(2):
        final.append(sums[half * RING])
        for d in range(1, RING):
            final.append(lax.ppermute(sums[half * RING + d], "gy", perms[half](-d)))
    out = call(place, [VMEM] * 8, shape(8, CHUNK, WIDTH))(*final)
    return out.reshape(tokens.shape)


def solution(mesh):
    return jax.shard_map(
        body,
        mesh=mesh,
        in_specs=(
            P("gx", "gy"),
            P("gy", "gx", None, None, None),
            P("gy", "gx", None, None, None),
            P("gy", "gx", None, None),
            P("gy", "gx"),
            P("gx", "gy", None, None, None),
            P("gx", None, None),
            P("gx", "gy", None, None),
            P("gx", "gy"),
        ),
        out_specs=P("gx", "gy"),
        check_vma=False,
    )
```

```python
import functools

import jax
import jax.numpy as jnp
from jax import lax
from jax.experimental import pallas as pl
from jax.experimental.pallas import tpu as pltpu
from jax.sharding import PartitionSpec as P


BLOCK = 128
SLOTS = 10
DOWN_SLOTS = 6
FB = 7
NZ = 8
RING = 4
GATE_ROWS = SLOTS * BLOCK
DOWN_AT = 2 * GATE_ROWS
META_AT = DOWN_AT + DOWN_SLOTS * BLOCK
MSG_ROWS = META_AT + 16
CHUNK = 32
SPLIT = 13 * BLOCK
TOP_UP = 3
N_MSGS = 10
N_TOKS = 7
WIDTH = 256
HID = 2 * FB


VMEM = pl.BlockSpec(memory_space=pltpu.VMEM)
HBM = pl.BlockSpec(memory_space=pltpu.HBM)
SMEM = pl.BlockSpec(memory_space=pltpu.SMEM)
bf16 = jnp.bfloat16


def z_perm(d):
    return [(2 * z + c, 2 * ((z + d) % NZ) + c) for z in range(NZ) for c in range(2)]


def x_perm(d):
    return [(4 * x + y, 4 * ((x + d) % 4) + y) for x in range(4) for y in range(4)]


def y_perm(d):
    return [(4 * x + y, 4 * x + (y + d) % 4) for x in range(4) for y in range(4)]


PARTNER = [(i, i ^ 1) for i in range(16)]


def plane_xy():
    me = lax.axis_index("gy")
    return lax.shift_right_logical(me, 2), me & 3


def send(x, axis, perm):
    return lax.ppermute(x, axis, perm)


def call(kernel, specs, out_shape, scratch=(), limit=16, flops=0):
    return pl.pallas_call(
        kernel,
        out_shape=out_shape,
        in_specs=specs,
        out_specs=jax.tree.map(lambda _: VMEM, out_shape),
        scratch_shapes=list(scratch),
        compiler_params=pltpu.CompilerParams(vmem_limit_bytes=limit << 20),
        cost_estimate=pl.CostEstimate(flops=flops, bytes_accessed=0, transcendentals=0),
    )


def shape(*dims, dtype=bf16):
    return jax.ShapeDtypeStruct(dims, dtype)


def split_tokens(tok, out):
    x, y = plane_xy()
    out[...] = jnp.zeros_like(out)
    for k in range(1, RING):
        u, w = (x + k) & 3, (y + k) & 3
        out[4 * u + y] = tok[u]
        out[4 * x + w] = tok[4 + w]


def stack_tokens(tok, got, out):
    x, y = plane_xy()
    out[0] = tok[x]
    out[RING] = tok[4 + y]
    for d in range(1, RING):
        out[d] = got[4 * ((x - d) & 3) + y]
        out[RING + d] = got[4 * x + ((y - d) & 3)]


def pass_on(m1, m2, p1, p2, up, dn):
    n = 2 * RING
    up[:n] = m1[...]
    up[n:] = m2[:RING]
    dn[:n] = p1[...]
    dn[n:] = p2[RING:]


def pack_weights(coords, count, rows, down_coords, down_count, gate, up, down, msg, sems):
    me = lax.axis_index("gy")
    copies = [
        pltpu.make_async_copy(gate, msg.at[pl.ds(0, GATE_ROWS)], sems.at[0]),
        pltpu.make_async_copy(up, msg.at[pl.ds(GATE_ROWS, GATE_ROWS)], sems.at[1]),
        pltpu.make_async_copy(down, msg.at[pl.ds(DOWN_AT, DOWN_SLOTS * BLOCK)], sems.at[2]),
    ]
    for c in copies:
        c.start()
    live = count[0, 0]
    down_live = down_count[0, 0]
    lane = lax.broadcasted_iota(jnp.int32, (16, BLOCK), 1)
    meta = jnp.zeros((16, BLOCK), jnp.int32)
    for s in range(SLOTS):
        meta = jnp.where(lane == s, coords[0, s] * FB + coords[1, s], meta)
    for s in range(DOWN_SLOTS):
        row = rows[down_coords[0, s], me]
        meta = jnp.where(lane == SLOTS + s, row * 2 + down_coords[1, s], meta)
    msg[META_AT:MSG_ROWS] = meta.astype(jnp.float32).astype(bf16)
    for c in copies:
        c.wait()
    zero = jnp.zeros((BLOCK, BLOCK), bf16)

    @pl.loop(live, SLOTS)
    def _(s):
        at = pl.multiple_of(s * BLOCK, BLOCK)
        msg[pl.ds(at, BLOCK), :] = zero
        msg[pl.ds(GATE_ROWS + at, BLOCK), :] = zero

    @pl.loop(down_live, DOWN_SLOTS)
    def _(s):
        msg[pl.ds(pl.multiple_of(DOWN_AT + s * BLOCK, BLOCK), BLOCK), :] = zero


def by_place(refs):
    found = []
    refs = list(refs)
    for d in range(RING):
        for core in range(2):
            upper = refs.pop(0) if d == 2 else None
            found.append((d, core, refs.pop(0), upper))
    return found


def read_places(msgs, at, slots):
    for i, (_, _, ref, upper) in enumerate(msgs):
        row = META_AT if upper is None else META_AT - SPLIT
        meta = ref[row : row + 16].astype(jnp.float32).astype(jnp.int32)
        for s in slots:
            at[i, s] = meta[0, s]


def gate_up(half, *refs):
    n = N_TOKS + N_MSGS
    own, m1, m2, up, dn, p2, p1 = refs[:N_TOKS]
    near = {0: own, 1: m1, 2: m2, 3: up, 5: dn, 6: p2, 7: p1}
    msgs, outs = by_place(refs[N_TOKS:n]), refs[n : n + RING]
    dense, lhs, at = refs[n + RING :]
    x, y = plane_xy()
    v = y if half == 0 else x
    for j in range(NZ):
        k = (j // 2 - v) & 3

        @pl.loop(0, RING)
        def _(d):
            at_d = pl.multiple_of(d * WIDTH, WIDTH)
            if j == 4:
                piece = (up, dn)[half][2 * RING + d]
            else:
                piece = near[j][half * RING + d]
            lhs[2 * k + j % 2, :, pl.ds(at_d, WIDTH)] = piece


    @pl.loop(0, HID)
    def _(n):
        dense[n] = jnp.zeros(dense.shape[1:], bf16)

    read_places(msgs, at, range(SLOTS))
    for i, (d, core, ref, upper) in enumerate(msgs):

        def put(src, base, lo, hi, lanes):
            def step(s, carry):
                p = at[i, s]
                r = (p >= FB).astype(jnp.int32)
                col = core * FB + p - FB * r
                row = pl.multiple_of(base + s * BLOCK, BLOCK)
                dense[col, 2 * d + r, :, lanes] = src[pl.ds(row, BLOCK), :]
                return carry

            lax.fori_loop(lo, hi, step, 0)

        gate, up = slice(0, BLOCK), slice(BLOCK, WIDTH)
        if upper is None:

            def both(s, carry):
                p = at[i, s]
                r = (p >= FB).astype(jnp.int32)
                col = core * FB + p - FB * r
                row = pl.multiple_of(s * BLOCK, BLOCK)
                dense[col, 2 * d + r, :, gate] = ref[pl.ds(row, BLOCK), :]
                dense[col, 2 * d + r, :, up] = ref[pl.ds(GATE_ROWS + row, BLOCK), :]
                return carry

            lax.fori_loop(0, SLOTS, both, 0, unroll=2)
        else:
            put(upper, 0, 0, SLOTS, gate)
            put(upper, GATE_ROWS, 0, TOP_UP, up)
            put(ref, GATE_ROWS - SPLIT, TOP_UP, SLOTS, up)

    left = lhs[...].reshape(NZ * CHUNK, RING * WIDTH)

    @pl.loop(0, HID)
    def _(n):
        part = jnp.dot(
            left, dense[n].reshape(RING * WIDTH, WIDTH), preferred_element_type=jnp.float32
        ).astype(bf16)
        for k in range(RING):
            outs[k][n] = part[2 * CHUNK * k : 2 * CHUNK * (k + 1)]


def activate(*refs):
    out = refs[RING]

    @pl.loop(0, HID)
    def _(n):
        total = refs[0][n].astype(jnp.float32)
        for k in range(1, RING):
            total = total + refs[k][n].astype(jnp.float32)
        gate, up = total[:, :BLOCK], total[:, BLOCK:]
        out[n] = (gate / (1.0 + jnp.exp(-gate)) * up).astype(bf16)


def spread_down(*refs):
    msgs, out, at = by_place(refs[:N_MSGS]), refs[N_MSGS], refs[N_MSGS + 1]

    @pl.loop(0, RING)
    def _(d):
        out[d] = jnp.zeros(out.shape[1:], bf16)

    read_places(msgs, at, range(SLOTS, SLOTS + DOWN_SLOTS))
    for i, (d, core, ref, upper) in enumerate(msgs):
        base = DOWN_AT if upper is None else DOWN_AT - SPLIT

        def step(s, carry):
            q = at[i, SLOTS + s]
            row = lax.shift_right_logical(q, 1)
            col = pl.multiple_of((q & 1) * BLOCK, BLOCK)
            src = pl.multiple_of(base + s * BLOCK, BLOCK)
            out[d, core * FB + row, :, pl.ds(col, BLOCK)] = ref[pl.ds(src, BLOCK), :]
            return carry

        lax.fori_loop(0, DOWN_SLOTS, step, 0)


def down(*refs):
    hids, dense, lefts = refs[: 2 * RING], refs[2 * RING : 2 * RING + 2], refs[17:]
    far_up, far_down, own, m1, m2, p2, p1 = refs[10:17]
    whole = {0: own, 1: m1, 2: m2, 3: far_down, 5: far_up, 6: p2, 7: p1}
    x, y = plane_xy()
    for half in range(2):
        v = y if half == 0 else x
        lhs = lefts[half]
        for d in range(RING):
            at = (v - d) & 3
            hid = hids[half * RING + d]

            @pl.loop(0, HID)
            def _(n):
                lhs[at, :, pl.ds(pl.multiple_of(n * BLOCK, BLOCK), BLOCK)] = hid[n]

    for half in range(2):
        left = lefts[half][...].reshape(NZ * CHUNK, HID * BLOCK)

        @pl.loop(0, RING)
        def _(d):
            part = jnp.dot(
                left,
                dense[half][d].reshape(HID * BLOCK, WIDTH),
                preferred_element_type=jnp.float32,
            ).astype(bf16)
            for j, ref in whole.items():
                ref[half * RING + d] = part[CHUNK * j : CHUNK * (j + 1)]
            (far_up, far_down)[half][2 * RING + d] = part[4 * CHUNK : 5 * CHUNK]


def relay(up, dn, m1, m2, p2, p1, out_m1, out_m2, out_p2, out_p1):
    def add(a, b):
        return (a.astype(jnp.float32) + b.astype(jnp.float32)).astype(bf16)

    @pl.loop(0, RING)
    def _(i):
        k = RING + i
        for b in (i, k):
            out_p1[b] = add(p1[b], up[b])
            out_m1[b] = add(m1[b], dn[b])
        out_p2[i] = add(p2[i], up[2 * RING + i])
        out_p2[k] = p2[k]
        out_m2[i] = m2[i]
        out_m2[k] = add(m2[k], dn[2 * RING + i])


def add_up(*refs):
    ins, outs = refs[:5], refs[5:]
    for i in range(2 * RING):
        total = ins[0][i].astype(jnp.float32)
        for ref in ins[1:]:
            total = total + ref[i].astype(jnp.float32)
        outs[i][...] = total.astype(bf16)


def place(*refs):
    out = refs[-1]
    x, y = plane_xy()
    for d in range(RING):
        out[(x + d) & 3] = refs[d][...]
        out[4 + ((y + d) & 3)] = refs[RING + d][...]


def body(
    tokens,
    gate_blocks,
    up_blocks,
    gate_coords,
    gate_count,
    down_blocks,
    down_rows,
    down_coords,
    down_count,
):
    perms = (x_perm, y_perm)

    tok = tokens.reshape(8, CHUNK, WIDTH)
    small = lax.all_to_all(
        call(split_tokens, [VMEM], shape(16, CHUNK, WIDTH))(tok),
        "gy", 0, 0, tiled=True,
    )
    mine = call(stack_tokens, [VMEM] * 2, shape(8, CHUNK, WIDTH))(tok, small)
    m1, m2, p2, p1 = [send(mine, "gx", z_perm(j)) for j in (1, 2, -2, -1)]
    up, dn = call(pass_on, [VMEM] * 4, [shape(12, CHUNK, WIDTH)] * 2)(m1, m2, p1, p2)
    toks = [mine, m1, m2, send(up, "gx", z_perm(2)), send(dn, "gx", z_perm(-2)), p2, p1]

    msg = call(
        pack_weights,
        [SMEM] * 5 + [HBM] * 3,
        shape(MSG_ROWS, BLOCK),
        scratch=[pltpu.SemaphoreType.DMA((3,))],
    )(
        gate_coords[0, 0].T,
        gate_count,
        down_rows[0].T,
        down_coords[0, 0].T,
        down_count,
        gate_blocks.reshape(GATE_ROWS, BLOCK),
        up_blocks.reshape(GATE_ROWS, BLOCK),
        down_blocks.reshape(DOWN_SLOTS * BLOCK, BLOCK),
    )
    own_pair = (msg, send(msg, "gx", PARTNER))
    weights = []
    for half in range(2):
        near = {d: send(msg, "gy", perms[half](d)) for d in (1, 3)}
        upper = send(near[1][:SPLIT], "gy", perms[half](1))
        lower = send(near[3][SPLIT:], "gy", perms[half](3))
        got = {1: near[1], 4: upper, 5: lower, 3: near[3]}
        swapped = {k: send(v, "gx", PARTNER) for k, v in got.items()}
        weights.append(
            [*own_pair, near[1], swapped[1], upper, lower, swapped[4], swapped[5], near[3], swapped[3]]
        )

    hidden = []
    dense_down = []
    for half in range(2):
        part = call(
            functools.partial(gate_up, half),
            [VMEM] * (N_TOKS + N_MSGS),
            [shape(HID, 2 * CHUNK, WIDTH)] * RING,
            scratch=[
                pltpu.VMEM((HID, 2 * RING, BLOCK, WIDTH), bf16),
                pltpu.VMEM((NZ, CHUNK, RING * WIDTH), bf16),
                pltpu.SMEM((2 * RING, SLOTS + DOWN_SLOTS), jnp.int32),
            ],
            limit=20,
            flops=2 * 256 * 1024 * 3584,
        )(*toks, *weights[half])
        got = [part[0]] + [send(part[d], "gy", perms[1 - half](d)) for d in range(1, RING)]
        dense_down.append(
            call(
                spread_down,
                [VMEM] * N_MSGS,
                shape(RING, HID, BLOCK, WIDTH),
                scratch=[pltpu.SMEM((2 * RING, SLOTS + DOWN_SLOTS), jnp.int32)],
                limit=12,
                flops=10**9,
            )(*weights[half])
        )
        h = call(activate, [VMEM] * RING, shape(HID, 2 * CHUNK, BLOCK))(*got)
        hidden += [h] + [send(h, "gy", perms[1 - half](d)) for d in range(1, RING)]
    shard = shape(8, CHUNK, WIDTH)
    far = shape(12, CHUNK, WIDTH)
    far_up, far_down, own, *near = call(
        down,
        [VMEM] * (2 * RING + 2),
        [far, far, shard, shard, shard, shard, shard],
        scratch=[pltpu.VMEM((RING, 2 * CHUNK, HID * BLOCK), bf16)] * 2,
        flops=2 * 2 * 256 * 1792 * 1024,
    )(*hidden, *dense_down)
    relayed = call(relay, [VMEM] * 6, [shard] * 4)(
        send(far_up, "gx", z_perm(2)), send(far_down, "gx", z_perm(-2)), *near
    )
    got = [own] + [send(part, "gx", z_perm(e)) for part, e in zip(relayed, (-1, -2, 2, 1))]
    sums = call(add_up, [VMEM] * 5, [shape(CHUNK, WIDTH)] * 8)(*got)
    final = []
    for half in range(2):
        final.append(sums[half * RING])
        for d in range(1, RING):
            final.append(send(sums[half * RING + d], "gy", perms[half](-d)))
    out = call(place, [VMEM] * 8, shape(8, CHUNK, WIDTH))(*final)
    return out.reshape(tokens.shape)


def solution(mesh):
    return jax.shard_map(
        body,
        mesh=mesh,
        in_specs=(
            P("gx", "gy"),
            P("gy", "gx", None, None, None),
            P("gy", "gx", None, None, None),
            P("gy", "gx", None, None),
            P("gy", "gx"),
            P("gx", "gy", None, None, None),
            P("gx", None, None),
            P("gx", "gy", None, None),
            P("gx", "gy"),
        ),
        out_specs=P("gx", "gy"),
        check_vma=False,
    )
```
